32 devices in a mesh: tok: 8 (over z, x), voc: 4 (over y, core).
Axes of the slice: x: 2, y: 2, z: 4, core: 2. Of those that a mesh axis runs over, the one named last changes fastest.
Arguments:
- hidden: bfloat16 [256, 3584], P('tok'), may hold values from -700 to 700
- teacher_logits: bfloat16 [256, 20480], P(None, ('tok', 'voc')), may hold values from -300 to 300
- sampled_ids: int32 [256], P('tok'), may hold values from 0 to 20479
- loss_mask: int32 [256], P('tok'), may hold values from 0 to 1, as said below
- student_head: bfloat16 [3584, 20480], P(None, ('tok', 'voc')), may hold values from -0.3125 to 0.3125
Outputs:
- loss: float32 [], replicated
- sampled_ratio: float32 [256], P(('tok', 'voc'))
- hidden_grad: bfloat16 [256, 3584], P(('tok', 'voc'))
- head_grad: bfloat16 [3584, 20480], P(None, ('tok', 'voc'))
The draws below stay inside these ranges and needn't reach their ends.
Inputs may be any that keep to these rules, and one draw needn't show every extreme that they name: `loss_mask`: at least one position is valid.
All inputs are finite; a program needn't handle non-finite values.
Results may differ from the reference program's by a relative error of at most 0.02.
Values may be sent and summed in bfloat16 or wider, within the bound.
A program may use at most 128 MiB of HBM per device.

```python
import jax
import jax.numpy as jnp

D = 3584
VOCAB = 20480
TOKENS = 256


def scaled_rows(key, row_count, col_count):
    base = jnp.clip(jax.random.normal(jax.random.fold_in(key, 1), (row_count, col_count), jnp.float32), -6.0, 6.0)
    return base


def draw_hidden(key, part):
    return scaled_rows(key, TOKENS, D).astype(jnp.bfloat16)


def draw_teacher_logits(key, part):
    base = 3.0 * jnp.clip(jax.random.normal(jax.random.fold_in(key, 21), (TOKENS, VOCAB), jnp.float32), -6.0, 6.0)
    return base.astype(jnp.bfloat16)


def draw_loss_mask(key, part):
    levels = jax.random.randint(jax.random.fold_in(key, 11), (TOKENS,), 0, 4)
    valid = jnp.where(levels < 3, 1, 0).astype(jnp.int32)
    position = jnp.arange(TOKENS, dtype=jnp.int32)
    return jnp.where(position == 0, 1, valid).astype(jnp.int32)


def plant(result, stream_key, least, high):
    longest = result.shape.index(max(result.shape))
    spots = []
    for shift in (0, 1):
        where = [jax.random.randint(jax.random.fold_in(stream_key, axis), (), 0, length) for axis, length in enumerate(result.shape)]
        where[longest] = (where[longest] + shift) % result.shape[longest]
        spots.append(tuple(where))
    return result.at[spots[0]].set(least).at[spots[1]].set(high)


def shard_levels(rng, dims, pieces, least, high):
    def one(dim, shards_of):
        draws = jax.random.uniform(jax.random.fold_in(jax.random.fold_in(rng, 6), dim), (shards_of,), jnp.float32, least / len(pieces), high / len(pieces))
        return jnp.repeat(jnp.exp(draws), dims[dim] // shards_of).reshape((-1,) + (1,) * (len(dims) - dim - 1))

    factor_of = one(*pieces[0])
    for cut in pieces[1:]:
        factor_of = factor_of * one(*cut)
    return factor_of


def bell_draw(key, shape, width, most, shards=(), kind=jnp.bfloat16):
    array = width * jax.random.normal(key, shape, jnp.float32)
    if shards:
        array = array * shard_levels(key, shape, shards, -0.22, 0.18)
    return jnp.clip(array, -most, most).astype(kind)


def setup_inputs(seed: int = 0) -> dict:
    key_of = jax.random.split(jax.random.key(seed), 6)
    hidden = draw_hidden(jax.random.fold_in(key_of[5], 71), 0)
    teacher_logits = draw_teacher_logits(jax.random.fold_in(key_of[5], 71), 0)
    sampled_ids = plant(jax.random.randint(key_of[2], (TOKENS,), 0, VOCAB), jax.random.fold_in(key_of[2], 1), 0, VOCAB - 1).astype(jnp.int32)
    loss_mask = draw_loss_mask(jax.random.fold_in(key_of[5], 71), 0)
    student_head = bell_draw(key_of[4], (D, VOCAB), (D // 9) ** -0.5, 0.3125, ((1, 32),))
    return {"hidden": hidden, "teacher_logits": teacher_logits, "sampled_ids": sampled_ids, "loss_mask": loss_mask, "student_head": student_head}


def reference(hidden, teacher_logits, sampled_ids, loss_mask, student_head):
    student = jnp.dot(hidden, student_head, preferred_element_type=jnp.float32)
    teacher = teacher_logits.astype(jnp.float32)
    student_log = jax.nn.log_softmax(student, axis=1)
    teacher_log = jax.nn.log_softmax(teacher, axis=1)
    probs = jnp.exp(student_log)
    differ = student_log - teacher_log
    row_kl = jnp.sum(probs * differ, axis=1)
    weight = loss_mask.astype(jnp.float32)
    count = jnp.sum(weight)
    loss = jnp.sum(weight * row_kl) / count
    picked = jnp.take_along_axis(differ, sampled_ids.astype(jnp.int32)[:, None], axis=1)[:, 0]
    dlogits = (weight[:, None] * probs * (differ - row_kl[:, None])).astype(jnp.bfloat16)
    hidden_grad = jnp.dot(dlogits, student_head.T, preferred_element_type=jnp.float32).astype(jnp.bfloat16)
    head_grad = jnp.dot(hidden.T, dlogits, preferred_element_type=jnp.float32).astype(jnp.bfloat16)
    return loss, picked, hidden_grad, head_grad
```

```python
import functools

import jax
import jax.numpy as jnp
from jax import lax
from jax.experimental import pallas as pl
from jax.experimental.pallas import tpu as pltpu
from jax.sharding import PartitionSpec as P

MESH = pl.DeviceIdType.MESH
F32 = jnp.float32
BF16 = jnp.bfloat16
LOW = -3.0e38


def columns_of(parts, rows):
    block = jnp.concatenate(parts + [jnp.zeros((8 - len(parts), rows), F32)], axis=0)
    block = jnp.concatenate([block, jnp.zeros((120, rows), F32)], axis=0)
    return jnp.transpose(block)


def rows_of(parts, rows):
    lane = lax.broadcasted_iota(jnp.int32, (rows, 128), 1)
    block = jnp.zeros((rows, 128), F32)
    for i, part in enumerate(parts):
        block = jnp.where(lane == i, part, block)
    return jnp.transpose(block)


def kernel(
    T, V, WA, WB, NCH,
    hidden, teacher_hbm, code_in, head_hbm,
    small_out, hgrad_out, wgrad_out,
    hid, head, teacher, code, student, tst, sst, cols, dl, dlp, acc,
    cs, cr, s1, r1, s2, r2, zs, zr, hg, wg,
    load_sem, zsem_s, zsem_r, xsem_s, xsem_r, ysem_s, ysem_r, csem_s, csem_r,
    code_s, code_r, ts_s, ts_r, ss_s, ss_r,
    rc_s, rc_r, r1_s, r1_r, r2_s, r2_r, rz_s, rz_r, wsem, osem,
):
    N = T * V
    G = T // 2
    RB, D = hidden.shape
    VD = head_hbm.shape[1]
    R = T * RB
    t, v = lax.axis_index("tok"), lax.axis_index("voc")
    me = t * V + v
    g, x = t // 2, t % 2
    y, c = v // 2, v % 2

    own_load = pltpu.make_async_copy(hidden, hid.at[t], load_sem.at[0])
    own_load.start()
    teacher_load = pltpu.make_async_copy(teacher_hbm, teacher, load_sem.at[1])
    teacher_load.start()
    code_load = pltpu.make_async_copy(code_in, code.at[t], load_sem.at[3])
    code_load.start()
    head_load = pltpu.make_async_copy(head_hbm, head, load_sem.at[2])
    head_load.start()

    barrier = pltpu.get_barrier_semaphore()

    def greet(j, carry):
        peer = lax.rem(me + j, N)
        pl.semaphore_signal(
            barrier, inc=1, device_id={"tok": peer // V, "voc": peer % V}, device_id_type=MESH
        )
        return carry

    lax.fori_loop(1, N, greet, 0)
    own_load.wait()
    code_load.wait()
    pl.semaphore_wait(barrier, N - 1)

    started = []

    def send(src, dst, s_sem, r_sem, to):
        copy = pltpu.make_async_remote_copy(
            src_ref=src, dst_ref=dst, send_sem=s_sem, recv_sem=r_sem,
            device_id=to, device_id_type=MESH,
        )
        copy.start()
        started.append(copy)
        return copy

    def a_cols(q):
        return pl.ds(pl.multiple_of(q * WA, 128), WA)

    def b_cols(q):
        return pl.ds(pl.multiple_of(V * WA + q * WB, 128), WB)

    def pieces(block):
        return (hid.at[block, :, a_cols(v)], hid.at[block, :, b_cols(c)])

    other_x = {"tok": g * 2 + 1 - x, "voc": v}
    other_y = {"tok": t, "voc": (1 - y) * 2 + c}
    other_c = {"tok": t, "voc": y * 2 + 1 - c}

    order = [1] + ([G - 1] if G > 2 else []) + list(range(2, G - 1))
    zcopies, xcopies, ycopies, ccopies = {}, {}, {}, {}
    for p, ref in enumerate(pieces(t)):
        xcopies[0, p] = send(ref, ref, xsem_s.at[0, p], xsem_r.at[0, p], other_x)
    for k in order:
        for p, ref in enumerate(pieces(t)):
            zcopies[k, p] = send(
                ref, ref, zsem_s.at[k, p], zsem_r.at[k, p],
                {"tok": lax.rem(g + k, G) * 2 + x, "voc": v},
            )

    def code_send(j, carry):
        pltpu.make_async_remote_copy(
            src_ref=code.at[t], dst_ref=code.at[t], send_sem=code_s.at[j], recv_sem=code_r.at[j],
            device_id={"tok": lax.rem(t + j, T), "voc": v}, device_id_type=MESH,
        ).start()
        return carry

    lax.fori_loop(1, T, code_send, 0)

    def exchange_start(buf, s_sems, r_sems):
        def body(j, carry):
            peer = lax.rem(me + j, N)
            pltpu.make_async_remote_copy(
                src_ref=buf.at[me], dst_ref=buf.at[me], send_sem=s_sems.at[j],
                recv_sem=r_sems.at[j],
                device_id={"tok": peer // V, "voc": peer % V}, device_id_type=MESH,
            ).start()
            return carry

        lax.fori_loop(1, N, body, 0)

    def exchange_wait(buf, s_sems, r_sems):
        def body(j, carry):
            source = lax.rem(me + N - j, N)
            pltpu.make_async_remote_copy(
                src_ref=buf.at[me], dst_ref=buf.at[source], send_sem=s_sems.at[j],
                recv_sem=r_sems.at[j],
                device_id={"tok": source // V, "voc": source % V}, device_id_type=MESH,
            ).wait()
            return carry

        lax.fori_loop(1, N, body, 0)

    teacher_load.wait()
    tl = teacher[...].astype(F32)
    t_max = jnp.max(tl, axis=1, keepdims=True)
    t_sum = jnp.sum(jnp.exp(tl - t_max), axis=1, keepdims=True)
    tst[me] = rows_of([t_max, t_sum], R)[0:2]
    exchange_start(tst, ts_s, ts_r)

    def landed(copies, key):
        copies[key].wait_recv()

    def forward(block, index, base, to_x):
        refs = pieces(block)
        if to_x:
            for p, ref in enumerate(refs):
                xcopies[index, p] = send(ref, ref, xsem_s.at[index, p], xsem_r.at[index, p], other_x)
        ref = refs[0]
        ycopies[base] = send(ref, ref, ysem_s.at[base], ysem_r.at[base], other_y)
        for p, ref in enumerate(refs):
            ccopies[base, p] = send(ref, ref, csem_s.at[base, p], csem_r.at[base, p], other_c)

    def x_landed(k):
        for p in range(2):
            landed(xcopies, (k, p))
        forward(lax.rem(g + G - k, G) * 2 + 1 - x, None, G + k, False)

    x_landed(0)
    for k in order:
        for p in range(2):
            landed(zcopies, (k, p))
        forward(lax.rem(g + G - k, G) * 2 + x, k, k, True)
    for k in order:
        x_landed(k)

    flat = hid.reshape(R, D)

    def part(where):
        return jnp.dot(flat[:, where], head[where, :], preferred_element_type=F32)

    head_load.wait()
    student[...] = part(a_cols(v)) + part(b_cols(c))
    for base in [G] + order + [G + k for k in order]:
        landed(ycopies, base)
        shift = base % G
        block = lax.rem(g + G - shift, G) * 2 + (x if base < G else 1 - x)
        ref = hid.at[block, :, a_cols((1 - y) * 2 + c)]
        ccopies[base, 2] = send(ref, ref, csem_s.at[base, 2], csem_r.at[base, 2], other_c)
        for p in range(2):
            landed(ccopies, (base, p))
    student[...] += part(a_cols((1 - y) * 2 + c))
    student[...] += part(a_cols(y * 2 + 1 - c)) + part(b_cols(1 - c))

    exchange_wait(tst, ts_s, ts_r)
    tm = tst[:, 0, :]
    tm_all = jnp.max(tm, axis=0, keepdims=True)
    ts_all = jnp.sum(jnp.exp(tm - tm_all) * tst[:, 1, :], axis=0, keepdims=True)
    tcol = columns_of([tm_all, jnp.log(ts_all)], R)
    lt = (teacher[...].astype(F32) - tcol[:, 0:1]) - tcol[:, 1:2]

    def code_wait(j, carry):
        source = lax.rem(t + T - j, T)
        pltpu.make_async_remote_copy(
            src_ref=code.at[t], dst_ref=code.at[source], send_sem=code_s.at[j],
            recv_sem=code_r.at[j], device_id={"tok": source, "voc": v}, device_id_type=MESH,
        ).wait()
        return carry

    lax.fori_loop(1, T, code_wait, 0)
    diagonal = lax.broadcasted_iota(jnp.int32, (RB, 128), 1) == lax.broadcasted_iota(
        jnp.int32, (RB, 128), 0
    )

    def column(row):
        return jnp.concatenate(
            [
                jnp.sum(jnp.where(diagonal, code[i, row : row + 1, :], 0.0), axis=1, keepdims=True)
                for i in range(T)
            ],
            axis=0,
        )

    ids = column(0)
    weight = column(1)
    mine = (me * VD + lax.broadcasted_iota(jnp.int32, (1, VD), 1)).astype(F32)
    chosen = ids == mine

    for base in [G] + order + [G + k for k in order]:
        landed(ccopies, (base, 2))
    s = student[...] + part(a_cols((1 - y) * 2 + 1 - c))
    student[...] = s
    s_max = jnp.max(s, axis=1, keepdims=True)
    rel = s - s_max
    e = jnp.exp(rel)
    diff = rel - lt
    s_sum = jnp.sum(e, axis=1, keepdims=True)
    cross = jnp.sum(e * diff, axis=1, keepdims=True)
    pick = jnp.max(jnp.where(chosen, diff, LOW), axis=1, keepdims=True)
    sst[me] = rows_of([s_max, s_sum, cross, pick], R)[0:4]
    exchange_start(sst, ss_s, ss_r)
    exchange_wait(sst, ss_s, ss_r)
    sm = sst[:, 0, :]
    ss = sst[:, 1, :]
    sm_all = jnp.max(sm, axis=0, keepdims=True)
    move = sm - sm_all
    scale = jnp.exp(move)
    total = jnp.sum(scale * ss, axis=0, keepdims=True)
    cross_all = jnp.sum(scale * (sst[:, 2, :] + ss * move), axis=0, keepdims=True)
    pick_all = jnp.max(sst[:, 3, :] + move, axis=0, keepdims=True)
    log_total = jnp.log(total)
    kl = cross_all / total - log_total
    ratio = pick_all - log_total
    scol = columns_of([sm_all, log_total, kl, ratio], R)
    kl_c = scol[:, 2:3]
    count = jnp.sum(weight, axis=0, keepdims=True)
    loss = jnp.sum(weight * kl_c, axis=0, keepdims=True) / count
    cols[...] = scol
    small_out[0] = cols[pl.ds(pl.multiple_of(me * (R // N), 8), R // N), :]
    small_out[1] = jnp.broadcast_to(loss, (R // N, 128))
    ls = (student[...] - scol[:, 0:1]) - scol[:, 1:2]
    d = weight * jnp.exp(ls) * ((ls - lt) - kl_c)
    dl[...] = d.astype(BF16)
    RO = R // N
    dlp[...] = (
        d.reshape(G, 2, 2, 2, RO, VD).transpose(3, 2, 1, 0, 4, 5).reshape(2, R // 2, VD).astype(BF16)
    )

    CW = D // NCH
    turns = [i for pair in zip(range(NCH // 2), range(NCH // 2, NCH)) for i in pair]
    H = R // 8
    other = ((1,), (1,))

    def grad_part(which, ch):
        return lax.dot_general(
            dlp[which], head[pl.ds(ch * CW, CW), :], (other, ((), ())), preferred_element_type=F32
        )

    hops = {}
    for ch in turns:
        cs[ch] = grad_part(1 - c, ch).astype(BF16)
        hops["c", ch] = send(cs.at[ch], cr.at[ch], rc_s.at[ch], rc_r.at[ch], other_c)
    for ch in turns:
        acc[ch] = grad_part(c, ch).reshape(2, 2, H, CW)
    wchunks = 7 if D % 7 == 0 else 1
    WC = D // wchunks
    wdone = []

    def weight_grad(i):
        rows = pl.ds(i * WC, WC)
        wg[rows, :] = lax.dot_general(
            flat[:, rows], dl[...], (((0,), (0,)), ((), ())), preferred_element_type=F32
        ).astype(BF16)
        copy = pltpu.make_async_copy(wg.at[rows, :], wgrad_out.at[rows, :], wsem.at[i])
        copy.start()
        wdone.append(copy)

    for ch in turns:
        hops["c", ch].wait_recv()
        acc[ch] += cr[ch].astype(F32).reshape(2, 2, H, CW)
        if ch < NCH // 2:
            s1[ch] = acc[ch, 1 - y].astype(BF16)
            to = other_y
        else:
            s1[ch] = acc[ch, :, 1 - x].astype(BF16)
            to = other_x
        hops["1", ch] = send(s1.at[ch], r1.at[ch], r1_s.at[ch], r1_r.at[ch], to)
    for i in range(0, 3 * wchunks // 7):
        weight_grad(i)
    for ch in turns:
        hops["1", ch].wait_recv()
        got = r1[ch].astype(F32)
        if ch < NCH // 2:
            acc[ch, y] += got
            s2[ch] = acc[ch, y, 1 - x].astype(BF16)
            to = other_x
        else:
            acc[ch, :, x] += got
            s2[ch] = acc[ch, 1 - y, x].astype(BF16)
            to = other_y
        hops["2", ch] = send(s2.at[ch], r2.at[ch], r2_s.at[ch], r2_r.at[ch], to)
    for i in range(3 * wchunks // 7, 5 * wchunks // 7):
        weight_grad(i)
    half = CW // 2
    for ch in turns:
        hops["2", ch].wait_recv()
        both = acc[ch, y, x] + r2[ch].astype(F32)
        for i in range(G):
            rows = both[i * RO : (i + 1) * RO]
            acc[ch, 0, 0, i * RO : (i + 1) * RO, :] = rows
            zs[ch, i] = jnp.concatenate([rows[:, :half], rows[:, half:]], axis=0).astype(BF16)
        for k in order:
            to = lax.rem(g + k, G)
            hops["z", ch, k] = send(
                zs.at[ch, to], zr.at[ch, k], rz_s.at[ch, k], rz_r.at[ch, k],
                {"tok": to * 2 + x, "voc": v},
            )
    for i in range(5 * wchunks // 7, wchunks):
        weight_grad(i)
    for ch in turns:
        mine_rows = acc[ch, 0, 0, pl.ds(pl.multiple_of(g * RO, 8), RO), :]
        for k in order:
            hops["z", ch, k].wait_recv()
            got = zr[ch, k].astype(F32)
            mine_rows = mine_rows + jnp.concatenate([got[:RO], got[RO:]], axis=1)
        hgrad_out[:, ch * CW : (ch + 1) * CW] = mine_rows.astype(BF16)
    for copy in started:
        copy.wait_send()
    for copy in wdone:
        copy.wait()


def per_device(T, V, hidden, teacher_logits, sampled_ids, loss_mask, student_head):
    RB, D = hidden.shape
    VD = student_head.shape[1]
    N, G, R = T * V, T // 2, T * RB
    RO = R // N
    units = D // 128
    a = (units * 5) // 28
    b = (units - V * a) // 2
    WA, WB = a * 128, b * 128
    NCH = 4
    CW = D // NCH
    code = jnp.pad(
        jnp.stack([sampled_ids, loss_mask]).astype(F32), ((0, 6), (0, 128 - RB))
    )
    DMA = pltpu.SemaphoreType.DMA
    H = R // 8
    any_space = pl.BlockSpec(memory_space=pl.ANY)
    vmem = pl.BlockSpec(memory_space=pltpu.VMEM)
    small, hidden_grad, head_grad = pl.pallas_call(
        functools.partial(kernel, T, V, WA, WB, NCH),
        out_shape=(
            jax.ShapeDtypeStruct((2, RO, 128), F32),
            jax.ShapeDtypeStruct((RO, D), BF16),
            jax.ShapeDtypeStruct((D, VD), BF16),
        ),
        in_specs=[any_space] * 4,
        out_specs=(vmem, vmem, any_space),
        scratch_shapes=[
            pltpu.VMEM((T, RB, D), BF16),
            pltpu.VMEM((D, VD), BF16),
            pltpu.VMEM((R, VD), BF16),
            pltpu.VMEM((T, 8, 128), F32),
            pltpu.VMEM((R, VD), F32),
            pltpu.VMEM((N, 2, R), F32),
            pltpu.VMEM((N, 4, R), F32),
            pltpu.VMEM((R, 128), F32),
            pltpu.VMEM((R, VD), BF16),
            pltpu.VMEM((2, R // 2, VD), BF16),
            pltpu.VMEM((NCH, 2, 2, H, CW), F32),
            pltpu.VMEM((NCH, R // 2, CW), BF16),
            pltpu.VMEM((NCH, R // 2, CW), BF16),
            pltpu.VMEM((NCH, 2, H, CW), BF16),
            pltpu.VMEM((NCH, 2, H, CW), BF16),
            pltpu.VMEM((NCH, H, CW), BF16),
            pltpu.VMEM((NCH, H, CW), BF16),
            pltpu.VMEM((NCH, G, 2 * RO, CW // 2), BF16),
            pltpu.VMEM((NCH, G, 2 * RO, CW // 2), BF16),
            pltpu.VMEM((8, 128), F32),
            pltpu.VMEM((D, VD), BF16),
            DMA((4,)),
            DMA((G, 2)), DMA((G, 2)),
            DMA((G, 2)), DMA((G, 2)),
            DMA((T,)), DMA((T,)),
            DMA((T, 3)), DMA((T, 3)),
            DMA((T,)), DMA((T,)),
            DMA((N,)), DMA((N,)),
            DMA((N,)), DMA((N,)),
            DMA((NCH,)), DMA((NCH,)),
            DMA((NCH,)), DMA((NCH,)),
            DMA((NCH,)), DMA((NCH,)),
            DMA((NCH, G)), DMA((NCH, G)),
            DMA((7,)),
            DMA((1,)),
        ],
        compiler_params=pltpu.CompilerParams(
            collective_id=0, has_side_effects=True, vmem_limit_bytes=60 * 1024 * 1024
        ),
    )(hidden, teacher_logits, code, student_head)
    return small[1, 0, 0], small[0, :, 3], hidden_grad, head_grad


def solution(mesh):
    in_specs = (
        P("tok", None),
        P(None, ("tok", "voc")),
        P("tok"),
        P("tok"),
        P(None, ("tok", "voc")),
    )
    out_specs = (P(), P(("tok", "voc")), P(("tok", "voc"), None), P(None, ("tok", "voc")))
    return jax.shard_map(
        functools.partial(per_device, mesh.shape["tok"], mesh.shape["voc"]),
        mesh=mesh, in_specs=in_specs, out_specs=out_specs, check_vma=False,
    )
```

```python
import functools

import jax
import jax.numpy as jnp
from jax import lax
from jax.experimental import pallas as pl
from jax.experimental.pallas import tpu as pltpu
from jax.sharding import PartitionSpec as P

MESH = pl.DeviceIdType.MESH
F32 = jnp.float32
BF16 = jnp.bfloat16
LOW = -3.0e38


def columns_of(parts, rows):
    block = jnp.concatenate(parts + [jnp.zeros((8 - len(parts), rows), F32)], axis=0)
    block = jnp.concatenate([block, jnp.zeros((120, rows), F32)], axis=0)
    return jnp.transpose(block)


def rows_of(parts, rows):
    lane = lax.broadcasted_iota(jnp.int32, (rows, 128), 1)
    block = jnp.zeros((rows, 128), F32)
    for i, part in enumerate(parts):
        block = jnp.where(lane == i, part, block)
    return jnp.transpose(block)


def kernel(
    T, V, WA, WB, NCH,
    hidden, teacher_hbm, ids_in, mask_in, head_hbm,
    loss_out, ratio_out, hgrad_out, wg,
    hid, head, teacher, code, student, tst, sst, cols, dl, dlp, acc,
    cs, cr, s1, r1, s2, r2, zs, zr,
    load_sem, zsem_s, zsem_r, xsem_s, xsem_r, ysem_s, ysem_r, csem_s, csem_r,
    kz_s, kz_r, kx_s, kx_r, ts_s, ts_r, ss_s, ss_r,
    rc_s, rc_r, r1_s, r1_r, r2_s, r2_r, rz_s, rz_r,
):
    N = T * V
    G = T // 2
    RB, D = hidden.shape
    VD = head_hbm.shape[1]
    R = T * RB
    t, v = lax.axis_index("tok"), lax.axis_index("voc")
    me = t * V + v
    g, x = t // 2, t % 2
    y, c = v // 2, v % 2

    own_load = pltpu.make_async_copy(hidden, hid.at[t], load_sem.at[0])
    own_load.start()
    teacher_load = pltpu.make_async_copy(teacher_hbm, teacher, load_sem.at[1])
    teacher_load.start()
    ids_load = pltpu.make_async_copy(ids_in, code.at[t, 0], load_sem.at[3])
    ids_load.start()
    mask_load = pltpu.make_async_copy(mask_in, code.at[t, 1], load_sem.at[4])
    mask_load.start()
    head_load = pltpu.make_async_copy(head_hbm, head, load_sem.at[2])
    head_load.start()

    barrier = pltpu.get_barrier_semaphore()

    other_x = {"tok": g * 2 + 1 - x, "voc": v}
    other_y = {"tok": t, "voc": (1 - y) * 2 + c}
    other_c = {"tok": t, "voc": y * 2 + 1 - c}

    def other_z(k):
        return {"tok": lax.rem(g + k, G) * 2 + x, "voc": v}

    for peer in [other_z(k) for k in range(1, G)] + [other_y, other_x, other_c]:
        pl.semaphore_signal(barrier, inc=1, device_id=peer, device_id_type=MESH)
    own_load.wait()
    ids_load.wait()
    mask_load.wait()
    pl.semaphore_wait(barrier, G + 2)

    started = []

    def send(src, dst, s_sem, r_sem, to):
        copy = pltpu.make_async_remote_copy(
            src_ref=src, dst_ref=dst, send_sem=s_sem, recv_sem=r_sem,
            device_id=to, device_id_type=MESH,
        )
        copy.start()
        started.append(copy)
        return copy

    def a_cols(q):
        return pl.ds(pl.multiple_of(q * WA, 128), WA)

    def b_cols(q):
        return pl.ds(pl.multiple_of(V * WA + q * WB, 128), WB)

    def pieces(block):
        return (hid.at[block, :, a_cols(v)], hid.at[block, :, b_cols(c)])

    order = [1] + ([G - 1] if G > 2 else []) + list(range(2, G - 1))
    zcopies, xcopies, ycopies, ccopies = {}, {}, {}, {}
    kzcopies, kxcopies = {}, {}

    def code_to_x(block, k):
        ref = code.at[block]
        kxcopies[k] = send(ref, ref, kx_s.at[k], kx_r.at[k], other_x)

    for p, ref in enumerate(pieces(t)):
        xcopies[0, p] = send(ref, ref, xsem_s.at[0, p], xsem_r.at[0, p], other_x)
    for k in order:
        for p, ref in enumerate(pieces(t)):
            zcopies[k, p] = send(
                ref, ref, zsem_s.at[k, p], zsem_r.at[k, p],
                other_z(k),
            )

    code_to_x(t, 0)
    for k in order:
        kzcopies[k] = send(code.at[t], code.at[t], kz_s.at[k], kz_r.at[k], other_z(k))

    def exchange_start(buf, s_sems, r_sems):
        def body(j, carry):
            peer = lax.rem(me + j, N)
            pltpu.make_async_remote_copy(
                src_ref=buf.at[me], dst_ref=buf.at[me], send_sem=s_sems.at[j],
                recv_sem=r_sems.at[j],
                device_id={"tok": peer // V, "voc": peer % V}, device_id_type=MESH,
            ).start()
            return carry

        lax.fori_loop(1, N, body, 0)

    def exchange_wait(buf, s_sems, r_sems):
        def body(j, carry):
            source = lax.rem(me + N - j, N)
            pltpu.make_async_remote_copy(
                src_ref=buf.at[me], dst_ref=buf.at[source], send_sem=s_sems.at[j],
                recv_sem=r_sems.at[j],
                device_id={"tok": source // V, "voc": source % V}, device_id_type=MESH,
            ).wait()
            return carry

        lax.fori_loop(1, N, body, 0)

    teacher_load.wait()
    tl = teacher[...].astype(F32)
    t_max = jnp.max(tl, axis=1, keepdims=True)
    t_sum = jnp.sum(jnp.exp(tl - t_max), axis=1, keepdims=True)
    tst[me] = rows_of([t_max, t_sum], R)[0:2]
    t_rel = tl - t_max

    def landed(copies, key):
        copies[key].wait_recv()

    def forward(block, index, base, to_x):
        refs = pieces(block)
        if to_x:
            for p, ref in enumerate(refs):
                xcopies[index, p] = send(ref, ref, xsem_s.at[index, p], xsem_r.at[index, p], other_x)
        ref = refs[0]
        ycopies[base] = send(ref, ref, ysem_s.at[base], ysem_r.at[base], other_y)
        for p, ref in enumerate(refs):
            ccopies[base, p] = send(ref, ref, csem_s.at[base, p], csem_r.at[base, p], other_c)

    def x_landed(k):
        for p in range(2):
            landed(xcopies, (k, p))
        forward(lax.rem(g + G - k, G) * 2 + 1 - x, None, G + k, False)

    x_landed(0)
    for k in order:
        for p in range(2):
            landed(zcopies, (k, p))
        forward(lax.rem(g + G - k, G) * 2 + x, k, k, True)
    for k in order:
        landed(kzcopies, k)
        code_to_x(lax.rem(g + G - k, G) * 2 + x, k)
    for k in order:
        x_landed(k)

    flat = hid.reshape(R, D)

    def part(where):
        return jnp.dot(flat[:, where], head[where, :], preferred_element_type=F32)

    head_load.wait()
    student[...] = part(a_cols(v)) + part(b_cols(c))
    for base in [G] + order + [G + k for k in order]:
        landed(ycopies, base)
        shift = base % G
        block = lax.rem(g + G - shift, G) * 2 + (x if base < G else 1 - x)
        ref = hid.at[block, :, a_cols((1 - y) * 2 + c)]
        ccopies[base, 2] = send(ref, ref, csem_s.at[base, 2], csem_r.at[base, 2], other_c)
        for p in range(2):
            landed(ccopies, (base, p))
    student[...] += part(a_cols((1 - y) * 2 + c))
    student[...] += part(a_cols(y * 2 + 1 - c)) + part(b_cols(1 - c))

    for k in [0] + order:
        landed(kxcopies, k)
    diagonal = lax.broadcasted_iota(jnp.int32, (RB, RB), 1) == lax.broadcasted_iota(
        jnp.int32, (RB, RB), 0
    )

    def column(row):
        return jnp.concatenate(
            [
                jnp.sum(jnp.where(diagonal, code[i, row].astype(F32), 0.0), axis=1, keepdims=True)
                for i in range(T)
            ],
            axis=0,
        )

    ids = column(0)
    weight = column(1)
    mine = (me * VD + lax.broadcasted_iota(jnp.int32, (1, VD), 1)).astype(F32)
    chosen = ids == mine

    for base in [G] + order + [G + k for k in order]:
        landed(ccopies, (base, 2))
    exchange_start(tst, ts_s, ts_r)
    s = student[...] + part(a_cols((1 - y) * 2 + 1 - c))
    student[...] = s
    s_max = jnp.max(s, axis=1, keepdims=True)
    rel = s - s_max
    e = jnp.exp(rel)
    diff = rel - t_rel
    s_sum = jnp.sum(e, axis=1, keepdims=True)
    cross = jnp.sum(e * diff, axis=1, keepdims=True)
    pick = jnp.max(jnp.where(chosen, diff, LOW), axis=1, keepdims=True)
    sst[me] = rows_of([s_max, s_sum, cross, pick], R)[0:4]
    exchange_start(sst, ss_s, ss_r)
    exchange_wait(tst, ts_s, ts_r)
    tm = tst[:, 0, :]
    tm_all = jnp.max(tm, axis=0, keepdims=True)
    tmove = tm - tm_all
    log_ts = jnp.log(jnp.sum(jnp.exp(tmove) * tst[:, 1, :], axis=0, keepdims=True))
    exchange_wait(sst, ss_s, ss_r)
    sm = sst[:, 0, :]
    ss = sst[:, 1, :]
    sm_all = jnp.max(sm, axis=0, keepdims=True)
    move = sm - sm_all
    scale = jnp.exp(move)
    total = jnp.sum(scale * ss, axis=0, keepdims=True)
    cross_all = jnp.sum(scale * (sst[:, 2, :] + ss * (move - tmove)), axis=0, keepdims=True)
    pick_all = jnp.max(sst[:, 3, :] + (move - tmove), axis=0, keepdims=True)
    log_total = jnp.log(total)
    kl = cross_all / total - log_total + log_ts
    ratio = pick_all - log_total + log_ts
    scol = columns_of([sm_all, log_total, kl, ratio, tm_all, log_ts], R)
    lt = (teacher[...].astype(F32) - scol[:, 4:5]) - scol[:, 5:6]
    kl_c = scol[:, 2:3]
    count = jnp.sum(weight, axis=0, keepdims=True)
    loss = jnp.sum(weight * kl_c, axis=0, keepdims=True) / count
    cols[...] = scol
    RO = R // N
    mine_col = cols[pl.ds(pl.multiple_of(me * RO, 8), RO), 3:4]
    eye = lax.broadcasted_iota(jnp.int32, (RO, RO), 1) == lax.broadcasted_iota(
        jnp.int32, (RO, RO), 0
    )
    ratio_out[...] = jnp.sum(jnp.where(eye, mine_col, 0.0), axis=0, keepdims=True)
    loss_out[...] = loss
    ls = (student[...] - scol[:, 0:1]) - scol[:, 1:2]
    d = weight * jnp.exp(ls) * ((ls - lt) - kl_c)
    dl[...] = d.astype(BF16)
    dlp[...] = (
        d.reshape(G, 2, 2, 2, RO, VD).transpose(3, 2, 1, 0, 4, 5).reshape(2, R // 2, VD).astype(BF16)
    )

    CW = D // NCH
    turns = [i for pair in zip(range(NCH // 2), range(NCH // 2, NCH)) for i in pair]
    H = R // 8
    other = ((1,), (1,))

    def grad_part(which, ch):
        return lax.dot_general(
            dlp[which], head[pl.ds(ch * CW, CW), :], (other, ((), ())), preferred_element_type=F32
        )

    hops = {}
    for ch in turns:
        cs[ch] = grad_part(1 - c, ch).astype(BF16)
        hops["c", ch] = send(cs.at[ch], cr.at[ch], rc_s.at[ch], rc_r.at[ch], other_c)
    for ch in turns:
        acc[ch] = grad_part(c, ch).reshape(2, 2, H, CW)
    wchunks = 7 if D % 7 == 0 else 1
    WC = D // wchunks

    def weight_grad(i):
        rows = pl.ds(i * WC, WC)
        wg[rows, :] = lax.dot_general(
            flat[:, rows], dl[...], (((0,), (0,)), ((), ())), preferred_element_type=F32
        ).astype(BF16)

    for ch in turns:
        hops["c", ch].wait_recv()
        acc[ch] += cr[ch].astype(F32).reshape(2, 2, H, CW)
        if ch < NCH // 2:
            s1[ch] = acc[ch, 1 - y].astype(BF16)
            to = other_y
        else:
            s1[ch] = acc[ch, :, 1 - x].astype(BF16)
            to = other_x
        hops["1", ch] = send(s1.at[ch], r1.at[ch], r1_s.at[ch], r1_r.at[ch], to)
    for i in range(0, 4 * wchunks // 7):
        weight_grad(i)
    half = CW // 2

    def second(ch):
        hops["1", ch].wait_recv()
        got = r1[ch].astype(F32)
        if ch < NCH // 2:
            acc[ch, y] += got
            s2[ch] = acc[ch, y, 1 - x].astype(BF16)
            to = other_x
        else:
            acc[ch, :, x] += got
            s2[ch] = acc[ch, 1 - y, x].astype(BF16)
            to = other_y
        hops["2", ch] = send(s2.at[ch], r2.at[ch], r2_s.at[ch], r2_r.at[ch], to)

    def third(ch):
        hops["2", ch].wait_recv()
        both = acc[ch, y, x] + r2[ch].astype(F32)
        acc[ch, 0, 0] = both
        for i in range(G):
            rows = both[i * RO : (i + 1) * RO]
            zs[ch, i] = jnp.concatenate([rows[:, :half], rows[:, half:]], axis=0).astype(BF16)
        for k in order:
            hops["z", ch, k] = send(
                zs.at[ch, lax.rem(g + k, G)], zr.at[ch, k], rz_s.at[ch, k], rz_r.at[ch, k],
                other_z(k),
            )

    lag = 4 if NCH > 4 else 2
    for i in range(NCH + lag):
        if i < NCH:
            second(turns[i])
        if i >= lag:
            third(turns[i - lag])
    for i in range(4 * wchunks // 7, wchunks):
        weight_grad(i)
    for ch in turns:
        mine_rows = acc[ch, 0, 0, pl.ds(pl.multiple_of(g * RO, 8), RO), :]
        for k in order:
            hops["z", ch, k].wait_recv()
            got = zr[ch, k].astype(F32)
            mine_rows = mine_rows + jnp.concatenate([got[:RO], got[RO:]], axis=1)
        hgrad_out[:, ch * CW : (ch + 1) * CW] = mine_rows.astype(BF16)
    for copy in started:
        copy.wait_send()


def store_all(a, b, c, d, oa, ob, oc, od, sem):
    copies = [
        pltpu.make_async_copy(src, dst, sem.at[i])
        for i, (src, dst) in enumerate(((d, od), (c, oc), (b, ob), (a, oa)))
    ]
    for copy in copies:
        copy.start()
    for copy in copies:
        copy.wait()


def per_device(T, V, hidden, teacher_logits, sampled_ids, loss_mask, student_head):
    RB, D = hidden.shape
    VD = student_head.shape[1]
    N, G, R = T * V, T // 2, T * RB
    RO = R // N
    units = D // 128
    a = (units * 5) // 28
    b = (units - V * a) // 2
    WA, WB = a * 128, b * 128
    NCH = D // 256 if (D // 256) % 2 == 0 else 2
    CW = D // NCH
    DMA = pltpu.SemaphoreType.DMA
    H = R // 8
    any_space = pl.BlockSpec(memory_space=pl.ANY)
    vmem = pl.BlockSpec(memory_space=pltpu.VMEM)
    shapes = (
        ((1, 1), F32), ((1, RO), F32), ((RO, D), BF16), ((D, VD), BF16),
    )
    kept = pl.pallas_call(
        functools.partial(kernel, T, V, WA, WB, NCH),
        out_shape=tuple(pltpu.VMEM(shape, kind) for shape, kind in shapes),
        in_specs=[any_space] * 5,
        out_specs=(vmem,) * 4,
        scratch_shapes=[
            pltpu.VMEM((T, RB, D), BF16),
            pltpu.VMEM((D, VD), BF16),
            pltpu.VMEM((R, VD), BF16),
            pltpu.VMEM((T, 2, 1, RB), jnp.int32),
            pltpu.VMEM((R, VD), F32),
            pltpu.VMEM((N, 2, R), F32),
            pltpu.VMEM((N, 4, R), F32),
            pltpu.VMEM((R, 128), F32),
            pltpu.VMEM((R, VD), BF16),
            pltpu.VMEM((2, R // 2, VD), BF16),
            pltpu.VMEM((NCH, 2, 2, H, CW), F32),
            pltpu.VMEM((NCH, R // 2, CW), BF16),
            pltpu.VMEM((NCH, R // 2, CW), BF16),
            pltpu.VMEM((NCH, 2, H, CW), BF16),
            pltpu.VMEM((NCH, 2, H, CW), BF16),
            pltpu.VMEM((NCH, H, CW), BF16),
            pltpu.VMEM((NCH, H, CW), BF16),
            pltpu.VMEM((NCH, G, 2 * RO, CW // 2), BF16),
            pltpu.VMEM((NCH, G, 2 * RO, CW // 2), BF16),
            DMA((5,)),
            DMA((G, 2)), DMA((G, 2)),
            DMA((G, 2)), DMA((G, 2)),
            DMA((T,)), DMA((T,)),
            DMA((T, 3)), DMA((T, 3)),
            DMA((G,)), DMA((G,)),
            DMA((G,)), DMA((G,)),
            DMA((N,)), DMA((N,)),
            DMA((N,)), DMA((N,)),
            DMA((NCH,)), DMA((NCH,)),
            DMA((NCH,)), DMA((NCH,)),
            DMA((NCH,)), DMA((NCH,)),
            DMA((NCH, G)), DMA((NCH, G)),
        ],
        compiler_params=pltpu.CompilerParams(
            collective_id=0, has_side_effects=True, vmem_limit_bytes=54 * 1024 * 1024
        ),
    )(
        hidden, teacher_logits, sampled_ids.reshape(1, RB), loss_mask.reshape(1, RB), student_head
    )
    loss, ratio, hidden_grad, head_grad = pl.pallas_call(
        store_all,
        out_shape=tuple(jax.ShapeDtypeStruct(shape, kind) for shape, kind in shapes),
        in_specs=[vmem] * 4,
        out_specs=(any_space,) * 4,
        scratch_shapes=[DMA((4,))],
        compiler_params=pltpu.CompilerParams(vmem_limit_bytes=1024 * 1024),
    )(*[pltpu.with_memory_space_constraint(part, pltpu.VMEM) for part in kept])
    return loss[0, 0], ratio[0], hidden_grad, head_grad


def solution(mesh):
    in_specs = (
        P("tok", None),
        P(None, ("tok", "voc")),
        P("tok"),
        P("tok"),
        P(None, ("tok", "voc")),
    )
    out_specs = (P(), P(("tok", "voc")), P(("tok", "voc"), None), P(None, ("tok", "voc")))
    return jax.shard_map(
        functools.partial(per_device, mesh.shape["tok"], mesh.shape["voc"]),
        mesh=mesh, in_specs=in_specs, out_specs=out_specs, check_vma=False,
    )
```

```python
import functools

import jax
import jax.numpy as jnp
from jax import lax
from jax.experimental import pallas as pl
from jax.experimental.pallas import tpu as pltpu
from jax.sharding import PartitionSpec as P

MESH = pl.DeviceIdType.MESH
F32 = jnp.float32
BF16 = jnp.bfloat16
LOW = -3.0e38


def columns_of(parts, rows):
    block = jnp.concatenate(parts + [jnp.zeros((8 - len(parts), rows), F32)], axis=0)
    block = jnp.concatenate([block, jnp.zeros((120, rows), F32)], axis=0)
    return jnp.transpose(block)


def rows_of(parts, rows):
    lane = lax.broadcasted_iota(jnp.int32, (rows, 128), 1)
    block = jnp.zeros((rows, 128), F32)
    for i, part in enumerate(parts):
        block = jnp.where(lane == i, part, block)
    return jnp.transpose(block)


def kernel(
    T, V, WA, WB, NCH,
    hidden, teacher_hbm, ids_in, mask_in, head_hbm,
    loss_out, ratio_out, hgrad_out, wg,
    hid, head, teacher, code, student, tst, sst, cols, dl, dlp, acc,
    cs, cr, s1, r1, s2, r2, zs, zr,
    load_sem, zsem_s, zsem_r, xsem_s, xsem_r, ysem_s, ysem_r, csem_s, csem_r,
    kz_s, kz_r, kx_s, kx_r, ts_s, ts_r, ss_s, ss_r,
    rc_s, rc_r, r1_s, r1_r, r2_s, r2_r, rz_s, rz_r,
):
    N = T * V
    G = T // 2
    RB, D = hidden.shape
    VD = head_hbm.shape[1]
    R = T * RB
    t, v = lax.axis_index("tok"), lax.axis_index("voc")
    me = t * V + v
    g, x = t // 2, t % 2
    y, c = v // 2, v % 2

    own_load = pltpu.make_async_copy(hidden, hid.at[t], load_sem.at[0])
    own_load.start()
    teacher_load = pltpu.make_async_copy(teacher_hbm, teacher, load_sem.at[1])
    teacher_load.start()
    ids_load = pltpu.make_async_copy(ids_in, code.at[t, 0], load_sem.at[3])
    ids_load.start()
    mask_load = pltpu.make_async_copy(mask_in, code.at[t, 1], load_sem.at[4])
    mask_load.start()
    head_load = pltpu.make_async_copy(head_hbm, head, load_sem.at[2])
    head_load.start()

    barrier = pltpu.get_barrier_semaphore()

    other_x = {"tok": g * 2 + 1 - x, "voc": v}
    other_y = {"tok": t, "voc": (1 - y) * 2 + c}
    other_c = {"tok": t, "voc": y * 2 + 1 - c}

    def other_z(k):
        return {"tok": lax.rem(g + k, G) * 2 + x, "voc": v}

    for peer in [other_z(k) for k in range(1, G)] + [other_y, other_x, other_c]:
        pl.semaphore_signal(barrier, inc=1, device_id=peer, device_id_type=MESH)
    own_load.wait()
    ids_load.wait()
    mask_load.wait()
    pl.semaphore_wait(barrier, G + 2)

    started = []

    def send(src, dst, s_sem, r_sem, to):
        copy = pltpu.make_async_remote_copy(
            src_ref=src, dst_ref=dst, send_sem=s_sem, recv_sem=r_sem,
            device_id=to, device_id_type=MESH,
        )
        copy.start()
        started.append(copy)
        return copy

    def a_cols(q):
        return pl.ds(pl.multiple_of(q * WA, 128), WA)

    def b_cols(q):
        return pl.ds(pl.multiple_of(V * WA + q * WB, 128), WB)

    def pieces(block):
        return (hid.at[block, :, a_cols(v)], hid.at[block, :, b_cols(c)])

    order = [1] + ([G - 1] if G > 2 else []) + list(range(2, G - 1))
    zcopies, xcopies, ycopies, ccopies = {}, {}, {}, {}
    kzcopies, kxcopies = {}, {}

    def code_to_x(block, k):
        ref = code.at[block]
        kxcopies[k] = send(ref, ref, kx_s.at[k], kx_r.at[k], other_x)

    for p, ref in enumerate(pieces(t)):
        xcopies[0, p] = send(ref, ref, xsem_s.at[0, p], xsem_r.at[0, p], other_x)
    for k in order:
        for p, ref in enumerate(pieces(t)):
            zcopies[k, p] = send(
                ref, ref, zsem_s.at[k, p], zsem_r.at[k, p],
                other_z(k),
            )

    code_to_x(t, 0)
    for k in order:
        kzcopies[k] = send(code.at[t], code.at[t], kz_s.at[k], kz_r.at[k], other_z(k))

    def exchange_start(buf, s_sems, r_sems):
        def body(j, carry):
            peer = lax.rem(me + j, N)
            pltpu.make_async_remote_copy(
                src_ref=buf.at[me], dst_ref=buf.at[me], send_sem=s_sems.at[j],
                recv_sem=r_sems.at[j],
                device_id={"tok": peer // V, "voc": peer % V}, device_id_type=MESH,
            ).start()
            return carry

        lax.fori_loop(1, N, body, 0)

    def exchange_wait(buf, s_sems, r_sems):
        def body(j, carry):
            source = lax.rem(me + N - j, N)
            pltpu.make_async_remote_copy(
                src_ref=buf.at[me], dst_ref=buf.at[source], send_sem=s_sems.at[j],
                recv_sem=r_sems.at[j],
                device_id={"tok": source // V, "voc": source % V}, device_id_type=MESH,
            ).wait()
            return carry

        lax.fori_loop(1, N, body, 0)

    teacher_load.wait()
    tl = teacher[...].astype(F32)
    t_max = jnp.max(tl, axis=1, keepdims=True)
    t_sum = jnp.sum(jnp.exp(tl - t_max), axis=1, keepdims=True)
    tst[me] = rows_of([t_max, t_sum], R)[0:2]
    t_rel = tl - t_max

    def landed(copies, key):
        copies[key].wait_recv()

    def forward(block, index, base, to_x):
        refs = pieces(block)
        if to_x:
            for p, ref in enumerate(refs):
                xcopies[index, p] = send(ref, ref, xsem_s.at[index, p], xsem_r.at[index, p], other_x)
        ref = refs[0]
        ycopies[base] = send(ref, ref, ysem_s.at[base], ysem_r.at[base], other_y)
        for p, ref in enumerate(refs):
            ccopies[base, p] = send(ref, ref, csem_s.at[base, p], csem_r.at[base, p], other_c)

    def x_landed(k):
        for p in range(2):
            landed(xcopies, (k, p))
        forward(lax.rem(g + G - k, G) * 2 + 1 - x, None, G + k, False)

    x_landed(0)
    for k in order:
        for p in range(2):
            landed(zcopies, (k, p))
        forward(lax.rem(g + G - k, G) * 2 + x, k, k, True)
    for k in order:
        landed(kzcopies, k)
        code_to_x(lax.rem(g + G - k, G) * 2 + x, k)
    for k in order:
        x_landed(k)

    flat = hid.reshape(R, D)

    def part(where):
        return jnp.dot(flat[:, where], head[where, :], preferred_element_type=F32)

    head_load.wait()
    student[...] = part(a_cols(v)) + part(b_cols(c))
    for base in [G] + order + [G + k for k in order]:
        landed(ycopies, base)
        shift = base % G
        block = lax.rem(g + G - shift, G) * 2 + (x if base < G else 1 - x)
        ref = hid.at[block, :, a_cols((1 - y) * 2 + c)]
        ccopies[base, 2] = send(ref, ref, csem_s.at[base, 2], csem_r.at[base, 2], other_c)
        for p in range(2):
            landed(ccopies, (base, p))
    student[...] += part(a_cols((1 - y) * 2 + c))
    student[...] += part(a_cols(y * 2 + 1 - c)) + part(b_cols(1 - c))

    for k in [0] + order:
        landed(kxcopies, k)
    diagonal = lax.broadcasted_iota(jnp.int32, (RB, RB), 1) == lax.broadcasted_iota(
        jnp.int32, (RB, RB), 0
    )

    def column(row):
        return jnp.concatenate(
            [
                jnp.sum(jnp.where(diagonal, code[i, row].astype(F32), 0.0), axis=1, keepdims=True)
                for i in range(T)
            ],
            axis=0,
        )

    ids = column(0)
    weight = column(1)
    mine = (me * VD + lax.broadcasted_iota(jnp.int32, (1, VD), 1)).astype(F32)
    chosen = ids == mine

    for base in [G] + order + [G + k for k in order]:
        landed(ccopies, (base, 2))
    exchange_start(tst, ts_s, ts_r)
    s = student[...] + part(a_cols((1 - y) * 2 + 1 - c))
    student[...] = s
    s_max = jnp.max(s, axis=1, keepdims=True)
    rel = s - s_max
    e = jnp.exp(rel)
    diff = rel - t_rel
    s_sum = jnp.sum(e, axis=1, keepdims=True)
    cross = jnp.sum(e * diff, axis=1, keepdims=True)
    pick = jnp.max(jnp.where(chosen, diff, LOW), axis=1, keepdims=True)
    sst[me] = rows_of([s_max, s_sum, cross, pick], R)[0:4]
    exchange_start(sst, ss_s, ss_r)
    exchange_wait(tst, ts_s, ts_r)
    tm = tst[:, 0, :]
    tm_all = jnp.max(tm, axis=0, keepdims=True)
    tmove = tm - tm_all
    log_ts = jnp.log(jnp.sum(jnp.exp(tmove) * tst[:, 1, :], axis=0, keepdims=True))
    exchange_wait(sst, ss_s, ss_r)
    sm = sst[:, 0, :]
    ss = sst[:, 1, :]
    sm_all = jnp.max(sm, axis=0, keepdims=True)
    move = sm - sm_all
    scale = jnp.exp(move)
    total = jnp.sum(scale * ss, axis=0, keepdims=True)
    cross_all = jnp.sum(scale * (sst[:, 2, :] + ss * (move - tmove)), axis=0, keepdims=True)
    pick_all = jnp.max(sst[:, 3, :] + (move - tmove), axis=0, keepdims=True)
    log_total = jnp.log(total)
    kl = cross_all / total - log_total + log_ts
    ratio = pick_all - log_total + log_ts
    scol = columns_of([sm_all, log_total, kl, ratio, tm_all, log_ts], R)
    lt = (teacher[...].astype(F32) - scol[:, 4:5]) - scol[:, 5:6]
    kl_c = scol[:, 2:3]
    count = jnp.sum(weight, axis=0, keepdims=True)
    loss = jnp.sum(weight * kl_c, axis=0, keepdims=True) / count
    cols[...] = scol
    RO = R // N
    mine_col = cols[pl.ds(pl.multiple_of(me * RO, 8), RO), 3:4]
    eye = lax.broadcasted_iota(jnp.int32, (RO, RO), 1) == lax.broadcasted_iota(
        jnp.int32, (RO, RO), 0
    )
    ratio_out[...] = jnp.sum(jnp.where(eye, mine_col, 0.0), axis=0, keepdims=True)
    loss_out[...] = loss
    ls = (student[...] - scol[:, 0:1]) - scol[:, 1:2]
    d = weight * jnp.exp(ls) * ((ls - lt) - kl_c)
    dl[...] = d.astype(BF16)
    dlp[...] = (
        d.reshape(G, 2, 2, 2, RO, VD).transpose(3, 2, 1, 0, 4, 5).reshape(2, R // 2, VD).astype(BF16)
    )

    CW = D // NCH
    turns = [i for pair in zip(range(NCH // 2), range(NCH // 2, NCH)) for i in pair]
    H = R // 8
    other = ((1,), (1,))

    def grad_part(which, ch):
        return lax.dot_general(
            dlp[which], head[pl.ds(ch * CW, CW), :], (other, ((), ())), preferred_element_type=F32
        )

    hops = {}
    for ch in turns:
        cs[ch] = grad_part(1 - c, ch).astype(BF16)
        hops["c", ch] = send(cs.at[ch], cr.at[ch], rc_s.at[ch], rc_r.at[ch], other_c)
    for ch in turns:
        acc[ch] = grad_part(c, ch).reshape(2, 2, H, CW)
    wchunks = 7 if D % 7 == 0 else 1
    WC = D // wchunks

    def weight_grad(i):
        rows = pl.ds(i * WC, WC)
        wg[rows, :] = lax.dot_general(
            flat[:, rows], dl[...], (((0,), (0,)), ((), ())), preferred_element_type=F32
        ).astype(BF16)

    for ch in turns:
        hops["c", ch].wait_recv()
        acc[ch] += cr[ch].astype(F32).reshape(2, 2, H, CW)
        if ch < NCH // 2:
            s1[ch] = acc[ch, 1 - y].astype(BF16)
            to = other_y
        else:
            s1[ch] = acc[ch, :, 1 - x].astype(BF16)
            to = other_x
        hops["1", ch] = send(s1.at[ch], r1.at[ch], r1_s.at[ch], r1_r.at[ch], to)
    for i in range(0, 4 * wchunks // 7):
        weight_grad(i)
    half = CW // 2

    def second(ch):
        hops["1", ch].wait_recv()
        got = r1[ch].astype(F32)
        if ch < NCH // 2:
            acc[ch, y] += got
            s2[ch] = acc[ch, y, 1 - x].astype(BF16)
            to = other_x
        else:
            acc[ch, :, x] += got
            s2[ch] = acc[ch, 1 - y, x].astype(BF16)
            to = other_y
        hops["2", ch] = send(s2.at[ch], r2.at[ch], r2_s.at[ch], r2_r.at[ch], to)

    def third(ch):
        hops["2", ch].wait_recv()
        both = acc[ch, y, x] + r2[ch].astype(F32)
        acc[ch, 0, 0] = both
        for i in range(G):
            rows = both[i * RO : (i + 1) * RO]
            zs[ch, i] = jnp.concatenate([rows[:, :half], rows[:, half:]], axis=0).astype(BF16)
        for k in order:
            hops["z", ch, k] = send(
                zs.at[ch, lax.rem(g + k, G)], zr.at[ch, k], rz_s.at[ch, k], rz_r.at[ch, k],
                other_z(k),
            )

    lag = NCH - 1
    for i in range(NCH + lag):
        if i < NCH:
            second(turns[i])
        if i >= lag:
            third(turns[i - lag])
    for i in range(4 * wchunks // 7, wchunks):
        weight_grad(i)
    for ch in turns:
        mine_rows = acc[ch, 0, 0, pl.ds(pl.multiple_of(g * RO, 8), RO), :]
        for k in order:
            hops["z", ch, k].wait_recv()
            got = zr[ch, k].astype(F32)
            mine_rows = mine_rows + jnp.concatenate([got[:RO], got[RO:]], axis=1)
        hgrad_out[:, ch * CW : (ch + 1) * CW] = mine_rows.astype(BF16)
    for copy in started:
        copy.wait_send()


def store_all(a, b, c, d, oa, ob, oc, od, sem):
    copies = [
        pltpu.make_async_copy(src, dst, sem.at[i])
        for i, (src, dst) in enumerate(((d, od), (c, oc), (b, ob), (a, oa)))
    ]
    for copy in copies:
        copy.start()
    for copy in copies:
        copy.wait()


def per_device(T, V, hidden, teacher_logits, sampled_ids, loss_mask, student_head):
    RB, D = hidden.shape
    VD = student_head.shape[1]
    N, G, R = T * V, T // 2, T * RB
    RO = R // N
    units = D // 128
    a = (units * 5) // 28
    b = (units - V * a) // 2
    WA, WB = a * 128, b * 128
    NCH = 4
    CW = D // NCH
    DMA = pltpu.SemaphoreType.DMA
    H = R // 8
    any_space = pl.BlockSpec(memory_space=pl.ANY)
    vmem = pl.BlockSpec(memory_space=pltpu.VMEM)
    shapes = (
        ((1, 1), F32), ((1, RO), F32), ((RO, D), BF16), ((D, VD), BF16),
    )
    kept = pl.pallas_call(
        functools.partial(kernel, T, V, WA, WB, NCH),
        out_shape=tuple(pltpu.VMEM(shape, kind) for shape, kind in shapes),
        in_specs=[any_space] * 5,
        out_specs=(vmem,) * 4,
        scratch_shapes=[
            pltpu.VMEM((T, RB, D), BF16),
            pltpu.VMEM((D, VD), BF16),
            pltpu.VMEM((R, VD), BF16),
            pltpu.VMEM((T, 2, 1, RB), jnp.int32),
            pltpu.VMEM((R, VD), F32),
            pltpu.VMEM((N, 2, R), F32),
            pltpu.VMEM((N, 4, R), F32),
            pltpu.VMEM((R, 128), F32),
            pltpu.VMEM((R, VD), BF16),
            pltpu.VMEM((2, R // 2, VD), BF16),
            pltpu.VMEM((NCH, 2, 2, H, CW), F32),
            pltpu.VMEM((NCH, R // 2, CW), BF16),
            pltpu.VMEM((NCH, R // 2, CW), BF16),
            pltpu.VMEM((NCH, 2, H, CW), BF16),
            pltpu.VMEM((NCH, 2, H, CW), BF16),
            pltpu.VMEM((NCH, H, CW), BF16),
            pltpu.VMEM((NCH, H, CW), BF16),
            pltpu.VMEM((NCH, G, 2 * RO, CW // 2), BF16),
            pltpu.VMEM((NCH, G, 2 * RO, CW // 2), BF16),
            DMA((5,)),
            DMA((G, 2)), DMA((G, 2)),
            DMA((G, 2)), DMA((G, 2)),
            DMA((T,)), DMA((T,)),
            DMA((T, 3)), DMA((T, 3)),
            DMA((G,)), DMA((G,)),
            DMA((G,)), DMA((G,)),
            DMA((N,)), DMA((N,)),
            DMA((N,)), DMA((N,)),
            DMA((NCH,)), DMA((NCH,)),
            DMA((NCH,)), DMA((NCH,)),
            DMA((NCH,)), DMA((NCH,)),
            DMA((NCH, G)), DMA((NCH, G)),
        ],
        compiler_params=pltpu.CompilerParams(
            collective_id=0, has_side_effects=True, vmem_limit_bytes=54 * 1024 * 1024
        ),
    )(
        hidden, teacher_logits, sampled_ids.reshape(1, RB), loss_mask.reshape(1, RB), student_head
    )
    loss, ratio, hidden_grad, head_grad = pl.pallas_call(
        store_all,
        out_shape=tuple(jax.ShapeDtypeStruct(shape, kind) for shape, kind in shapes),
        in_specs=[vmem] * 4,
        out_specs=(any_space,) * 4,
        scratch_shapes=[DMA((4,))],
        compiler_params=pltpu.CompilerParams(vmem_limit_bytes=1024 * 1024),
    )(*[pltpu.with_memory_space_constraint(part, pltpu.VMEM) for part in kept])
    return loss[0, 0], ratio[0], hidden_grad, head_grad


def solution(mesh):
    in_specs = (
        P("tok", None),
        P(None, ("tok", "voc")),
        P("tok"),
        P("tok"),
        P(None, ("tok", "voc")),
    )
    out_specs = (P(), P(("tok", "voc")), P(("tok", "voc"), None), P(None, ("tok", "voc")))
    return jax.shard_map(
        functools.partial(per_device, mesh.shape["tok"], mesh.shape["voc"]),
        mesh=mesh, in_specs=in_specs, out_specs=out_specs, check_vma=False,
    )
```
